32 devices in a mesh: hid: 2 (over x), wide: 16 (over z, y, core).
Axes of the slice: x: 2, y: 2, z: 4, core: 2. Of those that a mesh axis runs over, the one named last changes fastest.
Arguments:
- token_ids: int32 [2, 32, 128], P(None, 'hid'), may hold values from 0 to 152063, as said below
- segment_ids: int32 [2, 32, 128], P(None, ('hid', 'wide')), may hold values from 0 to 3, never falling along the last dimension, each value on 1 to 64 neighbouring positions
- step_ends: int32 [2, 32, 4], P(None, ('hid', 'wide')), may hold values from 0 to 127
- step_labels: int32 [2, 32, 4], P(None, 'hid'), may hold values from -1 to 2
- step_count: int32 [], replicated, may hold values from 2 to 20
- table: float32 [152064, 896], P(('hid', 'wide')), may hold values from -0.375 to 0.375
- attn_in: float32 [896, 1152], P('wide', 'hid'), may hold values from -0.1875 to 0.1875
- attn_out: float32 [896, 896], P('wide', 'hid'), may hold values from -0.078125 to 0.078125
- mlp_in: float32 [896, 2, 4864], P('wide', None, 'hid'), may hold values from -0.1875 to 0.1875
- mlp_out: float32 [4864, 896], P('hid', 'wide'), may hold values from -0.015625 to 0.015625
- small_params: float32 [3840], P(('hid', 'wide')), may hold values from -0.5 to 1.5
- table_first: float32 [152064, 896], P(('hid', 'wide')), may hold values from -1.1920929e-06 to 1.1920929e-06
- attn_in_first: float32 [896, 1152], P('wide', 'hid'), may hold values from -1.5258789e-05 to 1.5258789e-05
- attn_out_first: float32 [896, 896], P('wide', 'hid'), may hold values from -1.5258789e-05 to 1.5258789e-05
- mlp_in_first: float32 [896, 2, 4864], P('wide', None, 'hid'), may hold values from -4.7683716e-06 to 4.7683716e-06
- mlp_out_first: float32 [4864, 896], P('hid', 'wide'), may hold values from -7.6293945e-06 to 7.6293945e-06
- small_first: float32 [3840], P(('hid', 'wide')), may hold values from -0.00024414062 to 0.00024414062
- table_second: float32 [152064, 896], P(('hid', 'wide')), may hold values from 1.908266e-13 to 7.779854e-13
- attn_in_second: float32 [896, 1152], P('wide', 'hid'), may hold values from 2.5189113e-11 to 1.02694075e-10
- attn_out_second: float32 [896, 896], P('wide', 'hid'), may hold values from 3.2386e-11 to 1.3203523e-10
- mlp_in_second: float32 [896, 2, 4864], P('wide', None, 'hid'), may hold values from 2.9829212e-12 to 1.216114e-11
- mlp_out_second: float32 [4864, 896], P('hid', 'wide'), may hold values from 5.9658424e-12 to 2.432228e-11
- small_second: float32 [3840], P(('hid', 'wide')), may hold values from 6.7708332e-09 to 2.7604166e-08
Outputs:
- loss: float32 [], replicated
- grad_norm: float32 [], replicated
- table_new: float32 [152064, 896], P(('hid', 'wide'))
- table_first_new: float32 [152064, 896], P(('hid', 'wide'))
- table_second_new: float32 [152064, 896], P(('hid', 'wide'))
- attn_in_new: float32 [896, 1152], P('wide', 'hid')
- attn_in_first_new: float32 [896, 1152], P('wide', 'hid')
- attn_in_second_new: float32 [896, 1152], P('wide', 'hid')
- attn_out_new: float32 [896, 896], P('wide', 'hid')
- attn_out_first_new: float32 [896, 896], P('wide', 'hid')
- attn_out_second_new: float32 [896, 896], P('wide', 'hid')
- mlp_in_new: float32 [896, 2, 4864], P('wide', None, 'hid')
- mlp_in_first_new: float32 [896, 2, 4864], P('wide', None, 'hid')
- mlp_in_second_new: float32 [896, 2, 4864], P('wide', None, 'hid')
- mlp_out_new: float32 [4864, 896], P('hid', 'wide')
- mlp_out_first_new: float32 [4864, 896], P('hid', 'wide')
- mlp_out_second_new: float32 [4864, 896], P('hid', 'wide')
- small_new: float32 [3840], P(('hid', 'wide'))
- small_first_new: float32 [3840], P(('hid', 'wide'))
- small_second_new: float32 [3840], P(('hid', 'wide'))
The draws below stay inside these ranges and needn't reach their ends.
Inputs may be any that keep to these rules, and one draw needn't show every extreme that they name: `token_ids`: call id // 4752 the block of an id; in every sequence at most 16 tokens have blocks with the same remainder modulo 16, and in every sequence some remainder has exactly 16 of them.
All inputs are finite; a program needn't handle non-finite values.
Results may differ from the reference program's by a relative error of at most 0.02.
Values may be sent and summed in bfloat16 or wider, within the bound.
A program may use at most 224 MiB of HBM per device.

```python
import math
import jax
import jax.numpy as jnp
import numpy as np
from jax import lax

D = 896
HEADS = 14
KV_HEADS = 2
HEAD = 64
FF = 4864
VOCAB = 152064
SEQ = 128
MB = 2
SLOTS = 4
SEQS = 32
SLICES = 16
BLOCK = 4752
CAP = 16
ATT = 896
QKVW = 1152
GROUP = 7
SMALL = 3840


def draw_small_params(key, part):
    gain_key, bias_key = jax.random.split(jax.random.fold_in(key, 7))
    gain_part = jax.random.uniform(gain_key, (3 * D,), jnp.float32, 0.6, 1.4)
    bias_part = jnp.clip(0.1 * jax.random.normal(bias_key, (QKVW,), jnp.float32), -0.5, 0.5)
    return jnp.concatenate([gain_part, bias_part]).astype(jnp.float32)


def draw_token_ids(key, part):

    def one_row(row_key):
        star_key, order_key, shuffle_key, upper_key, inner_key, second_key = jax.random.split(row_key, 6)
        star = jax.random.randint(star_key, (), 0, SLICES)
        pool = jnp.arange(SLICES * CAP, dtype=jnp.int32) // CAP
        order = jax.random.permutation(order_key, SLICES * CAP).astype(jnp.int32)
        score = jnp.where(pool == star, order - SLICES * CAP, order)
        chosen = pool[jnp.argsort(score, stable=True)][:SEQ]
        holders = jax.random.permutation(shuffle_key, chosen)
        upper = jax.random.randint(upper_key, (SEQ,), 0, SEQS // SLICES)
        inner = jnp.minimum(jax.random.randint(inner_key, (SEQ,), 0, BLOCK), jax.random.randint(second_key, (SEQ,), 0, BLOCK))
        return ((upper * SLICES + holders) * BLOCK + inner).astype(jnp.int32)
    rows = jax.vmap(one_row)(jax.random.split(jax.random.fold_in(key, 11), MB * SEQS))
    return rows.reshape(MB, SEQS, SEQ)


def set_ends(values, key, smallest, largest):
    dims = values.shape
    index_at = [jax.random.randint(jax.random.fold_in(key, axis), (), 0, dims[axis]) for axis in range(len(dims))]
    values = values.at[tuple(index_at)].set(smallest)
    longest = dims.index(max(dims))
    index_at[longest] = (index_at[longest] + 1) % dims[longest]
    return values.at[tuple(index_at)].set(largest)


def block_scale(stream_key, shape, cuts, smallest, top_value):
    factor_of = 1.0
    for axis_at, blocks in cuts:
        heights = jax.random.uniform(jax.random.fold_in(jax.random.fold_in(stream_key, 6), axis_at), (blocks,), jnp.float32, smallest / len(cuts), top_value / len(cuts))
        factor_of = factor_of * jnp.repeat(jnp.exp(heights), shape[axis_at] // blocks).reshape((-1,) + (1,) * (len(shape) - 1 - axis_at))
    return factor_of


def length_profile(number_of, total, reach, slope):
    weights = [(1 << 20) // math.isqrt(standing ** slope) + 1 for standing in range(2, number_of + 1)]
    spare, holding = total - reach - (number_of - 1), [1] * (number_of - 1)
    while spare > 0:
        movable = [i for i in range(number_of - 1) if holding[i] < reach]
        mass, remaining = sum([weights[i] for i in movable]), spare
        for i in movable:
            addition = min(reach - holding[i], max(1, remaining * weights[i] // mass), spare)
            holding[i] = holding[i] + addition
            spare = spare - addition
    return np.array([reach] + holding)


def uneven_parts(key, count, total, most, slope):
    if count == 2:
        one = jax.random.randint(key, (), max(1, total - most), min(most, total - 1) + 1)
        return jnp.stack([one, total - one])
    lengths = jnp.asarray(length_profile(count, total, most, slope), jnp.int32)
    couples = (count - 1) // 2
    source_of, receiver = lengths[1:1 + 2 * couples:2], lengths[2:2 + 2 * couples:2]
    room = jnp.minimum(source_of - 1, most - receiver)
    moved = jax.random.randint(jax.random.fold_in(key, 1), (couples,), 0, 1 << 20) % (room + 1)
    lengths = lengths.at[1:1 + 2 * couples:2].set(source_of - moved).at[2:2 + 2 * couples:2].set(receiver + moved)
    return lengths[jax.random.permutation(jax.random.fold_in(key, 2), count)]


def centred(rng, shape, width, limit, pieces=(), held_as=jnp.bfloat16):
    array = width * jax.random.normal(rng, shape, jnp.float32)
    if pieces:
        array = array * block_scale(rng, shape, pieces, -0.22, 0.18)
    return jnp.clip(array, -limit, limit).astype(held_as)


def setup_inputs(seed: int = 0) -> dict:
    key_of = jax.random.split(jax.random.key(seed), 24)
    return {
        "token_ids": draw_token_ids(jax.random.fold_in(key_of[23], 71), 0),
        "segment_ids": jax.vmap(lambda own: jnp.searchsorted(jnp.cumsum(uneven_parts(own, 4, SEQ, SEQ // 2, 2)), jnp.arange(SEQ), side="right"))(jax.random.split(key_of[1], MB * SEQS)).reshape((MB, SEQS, SEQ)).astype(jnp.int32),
        "step_ends": set_ends(jax.random.randint(key_of[2], (MB, SEQS, SLOTS), 0, SEQ), jax.random.fold_in(key_of[2], 1), 0, SEQ - 1).astype(jnp.int32),
        "step_labels": set_ends(jax.random.randint(key_of[3], (MB, SEQS, SLOTS), -1, 3), jax.random.fold_in(key_of[3], 1), -1, 2).astype(jnp.int32),
        "step_count": jax.random.randint(key_of[4], (), 2, 21).astype(jnp.int32),
        "table": centred(key_of[5], (VOCAB, D), (2.0 / D ** 0.5), 0.375, ((0, 32),), jnp.float32),
        "attn_in": centred(key_of[6], (D, QKVW), D ** -0.5, 0.1875, ((0, 16), (1, 2)), jnp.float32),
        "attn_out": centred(key_of[7], (ATT, D), (0.4 / ATT ** 0.5), 0.078125, ((0, 16), (1, 2)), jnp.float32),
        "mlp_in": centred(key_of[8], (D, 2, FF), D ** -0.5, 0.1875, ((0, 16), (2, 2)), jnp.float32),
        "mlp_out": centred(key_of[9], (FF, D), (0.2 / FF ** 0.5), 0.015625, ((0, 2), (1, 16)), jnp.float32),
        "small_params": draw_small_params(jax.random.fold_in(key_of[23], 71), 0),
        "table_first": centred(key_of[11], (VOCAB, D), (0.0055 / (5 * VOCAB * D) ** 0.5), 1.1920928955078125e-06, ((0, 32),), jnp.float32),
        "attn_in_first": centred(key_of[12], (D, QKVW), (0.0055 / (5 * D * QKVW) ** 0.5), 1.52587890625e-05, ((0, 16), (1, 2)), jnp.float32),
        "attn_out_first": centred(key_of[13], (ATT, D), (0.0055 / (5 * ATT * D) ** 0.5), 1.52587890625e-05, ((0, 16), (1, 2)), jnp.float32),
        "mlp_in_first": centred(key_of[14], (D, 2, FF), (0.0055 / (10 * D * FF) ** 0.5), 4.76837158203125e-06, ((0, 16), (2, 2)), jnp.float32),
        "mlp_out_first": centred(key_of[15], (FF, D), (0.0055 / (5 * FF * D) ** 0.5), 7.62939453125e-06, ((0, 2), (1, 16)), jnp.float32),
        "small_first": centred(key_of[16], (SMALL,), (0.0055 / (5 * SMALL) ** 0.5), 0.00024414062, ((0, 32),), jnp.float32),
        "table_second": jnp.clip(jnp.exp(math.log(7.779854234793437e-13) - 1.4053426 * jax.random.uniform(key_of[17], (VOCAB, D), jnp.float32) ** block_scale(key_of[17], (VOCAB, D), ((0, 32),), -0.2, 0.2)), 1.9082660256651562e-13, 7.779854234793437e-13),
        "attn_in_second": jnp.clip(jnp.exp(math.log(1.026940754655925e-10) - 1.4053426 * jax.random.uniform(key_of[18], (D, QKVW), jnp.float32) ** block_scale(key_of[18], (D, QKVW), ((0, 16), (1, 2)), -0.2, 0.2)), 2.5189112948242887e-11, 1.026940754655925e-10),
        "attn_out_second": jnp.clip(jnp.exp(math.log(1.3203522997162764e-10) - 1.40534255 * jax.random.uniform(key_of[19], (ATT, D), jnp.float32) ** block_scale(key_of[19], (ATT, D), ((0, 16), (1, 2)), -0.2, 0.2)), 3.2386000131667814e-11, 1.3203522997162764e-10),
        "mlp_in_second": jnp.clip(jnp.exp(math.log(1.2161140150457328e-11) - 1.40534255 * jax.random.uniform(key_of[20], (D, 2, FF), jnp.float32) ** block_scale(key_of[20], (D, 2, FF), ((0, 16), (2, 2)), -0.2, 0.2)), 2.982921201710731e-12, 1.2161140150457328e-11),
        "mlp_out_second": jnp.clip(jnp.exp(math.log(2.4322280300914656e-11) - 1.40534255 * jax.random.uniform(key_of[21], (FF, D), jnp.float32) ** block_scale(key_of[21], (FF, D), ((0, 2), (1, 16)), -0.2, 0.2)), 5.965842403421462e-12, 2.4322280300914656e-11),
        "small_second": jnp.clip(jnp.exp(math.log(2.7604166064065794e-08) - 1.40534255 * jax.random.uniform(key_of[22], (SMALL,), jnp.float32) ** block_scale(key_of[22], (SMALL,), ((0, 32),), -0.2, 0.2)), 6.7708332274207805e-09, 2.7604166064065794e-08),
    }


@jax.custom_vjp
def low(v):
    return lax.optimization_barrier(v.astype(jnp.bfloat16)).astype(jnp.float32)

@jax.custom_vjp
def low_back(v):
    return v

def low_keep(v):
    return (low(v), None)

def low_pass(kept, grad):
    return (grad,)

def back_keep(v):
    return (v, None)

def back_low(kept, grad):
    return (low(grad),)
low.defvjp(low_keep, low_pass)
low_back.defvjp(back_keep, back_low)
norm_eps = 1e-06
rope_base = 1000000.0
plus_token = 10
minus_token = 12
clip_limit = 0.05
beta_one = 0.9
beta_two = 0.95
adam_eps = 1e-08
decay_rate = 0.1
rates = (0.03, 0.015, 0.015, 0.015, 0.0015, 0.3)
highest = lax.Precision.HIGHEST

def rms_scale(rows, gain):
    return rows * lax.rsqrt(lax.optimization_barrier(jnp.mean(rows * rows, axis=-1, keepdims=True)) + norm_eps) * gain

def positions_of(segment):
    places = jnp.arange(segment.shape[0], dtype=jnp.int32)
    starts = jnp.concatenate([jnp.ones((1,), dtype=bool), segment[1:] != segment[:-1]])
    opening = lax.cummax(jnp.where(starts, places, 0), axis=0)
    return (places - opening).astype(jnp.float32)

def angles_of(positions):
    half_size = HEAD // 2
    frequency = rope_base ** (-jnp.arange(half_size, dtype=jnp.float32) / half_size)
    return positions[:, None] * frequency[None, :]

def rotate(values, angles, sign):
    half_size = values.shape[-1] // 2
    cosine = jnp.cos(angles)[:, None, :]
    sine_part = sign * jnp.sin(angles)[:, None, :]
    leading = values[..., :half_size]
    trailing = values[..., half_size:]
    return jnp.concatenate([leading * cosine - trailing * sine_part, trailing * cosine + leading * sine_part], axis=-1)

def causal_mask(segment):
    places = jnp.arange(segment.shape[0])
    return (segment[:, None] == segment[None, :]) & (places[:, None] >= places[None, :])

def sequence_forward(embedded, segment, weight_in, weight_out, gate_up, weight_down, gains, bias):
    length = embedded.shape[0]
    normed = low(rms_scale(embedded, gains[0]))
    linear = low_back(jnp.dot(normed, weight_in, precision=highest) + bias)
    angles = angles_of(positions_of(segment))
    queries = linear[:, :ATT].reshape(length, HEADS, HEAD)
    keys = linear[:, ATT:ATT + KV_HEADS * HEAD].reshape(length, KV_HEADS, HEAD)
    values = low(linear[:, ATT + KV_HEADS * HEAD:].reshape(length, KV_HEADS, HEAD))
    queries = low(rotate(queries, angles, 1.0)).reshape(length, KV_HEADS, GROUP, HEAD)
    keys = low(rotate(keys, angles, 1.0))
    scores = low_back(jnp.einsum('skgd,tkd->kgst', queries, keys, precision=highest)) * HEAD ** (-0.5)
    scores = jnp.where(causal_mask(segment)[None, None], scores, -1e+30)
    probs = jax.nn.softmax(scores, axis=-1)
    mixed = jnp.einsum('kgst,tkd->skgd', low(probs), values, precision=highest).reshape(length, ATT)
    mixed = low(low_back(mixed))
    hidden_one = embedded + low_back(jnp.dot(mixed, weight_out, precision=highest))
    normed_two = low(rms_scale(hidden_one, gains[1]))
    gate = low_back(jnp.dot(normed_two, gate_up[:, 0], precision=highest))
    upward = low_back(jnp.dot(normed_two, gate_up[:, 1], precision=highest))
    inner = low(jax.nn.silu(gate) * upward)
    return hidden_one + low_back(jnp.dot(inner, weight_down, precision=highest))

def block_loss(rounded, block_data):
    table, weight_in, weight_out, gate_up, weight_down, smalls = rounded
    block_ids, block_segments, block_ends, block_labels = block_data
    gains = smalls[:3 * D].reshape(3, D)
    bias = smalls[3 * D:]
    embedded = low_back(table[block_ids])
    forward_one = jax.vmap(sequence_forward, in_axes=(0, 0, None, None, None, None, None, None))
    final_rows = forward_one(embedded, block_segments, weight_in, weight_out, gate_up, weight_down, gains, bias)
    picked = jnp.take_along_axis(final_rows, block_ends[:, :, None], axis=1)
    normed = low(rms_scale(picked, gains[2]))
    logits = low_back(jnp.einsum('bsd,vd->bsv', normed, table, precision=highest))
    totals = jax.nn.logsumexp(logits, axis=-1)
    target = jnp.where(block_labels >= 1, plus_token, minus_token).astype(jnp.int32)
    chosen = jnp.take_along_axis(logits, target[:, :, None], axis=2)[:, :, 0]
    return jnp.sum(jnp.where(block_labels >= 0, totals - chosen, 0.0))

def reference(token_ids, segment_ids, step_ends, step_labels, step_count, table, attn_in, attn_out, mlp_in, mlp_out, small_params, table_first, attn_in_first, attn_out_first, mlp_in_first, mlp_out_first, small_first, table_second, attn_in_second, attn_out_second, mlp_in_second, mlp_out_second, small_second):
    total_rows = MB * SEQS
    block = math.gcd(max(1, 4096 // SEQ), total_rows)

    def shaped(values):
        return values.reshape((total_rows // block, block) + values.shape[2:])
    data = (shaped(token_ids), shaped(segment_ids), shaped(step_ends), shaped(step_labels))
    masters = (table, attn_in, attn_out, mlp_in, mlp_out, small_params)
    firsts = (table_first, attn_in_first, attn_out_first, mlp_in_first, mlp_out_first, small_first)
    seconds = (table_second, attn_in_second, attn_out_second, mlp_in_second, mlp_out_second, small_second)

    def loss_sum(params):
        rounded = tuple((low(item) for item in params))

        def scan_step(carry, block_data):
            return (carry + jax.checkpoint(block_loss)(rounded, block_data), None)
        result, unused = lax.scan(scan_step, jnp.zeros((), jnp.float32), data)
        return result
    value, pullback = jax.vjp(loss_sum, masters)
    grads, = pullback(jnp.ones((), jnp.float32))
    count = jnp.sum((step_labels >= 0).astype(jnp.float32))
    denom = jnp.maximum(count, 1.0)
    grads = tuple((item / denom for item in grads))
    grad_norm = jnp.sqrt(sum((jnp.sum(item * item) for item in grads)))
    factor = clip_limit / jnp.maximum(grad_norm, clip_limit)
    step_value = step_count.astype(jnp.float32)
    bias_one = 1.0 - beta_one ** step_value
    bias_two = 1.0 - beta_two ** step_value
    results = [value / denom, grad_norm]
    for grad_total, weight_old, first_old, second_old, step_rate in zip(grads, masters, firsts, seconds, rates):
        clipped = grad_total * factor
        first_new = beta_one * first_old + (1.0 - beta_one) * clipped
        second_new = beta_two * second_old + (1.0 - beta_two) * clipped * clipped
        update = first_new / bias_one / (jnp.sqrt(second_new / bias_two) + adam_eps) + decay_rate * weight_old
        results += [weight_old - step_rate * update, first_new, second_new]
    return (results[0], results[1], results[2], results[3], results[4], results[5], results[6], results[7], results[8], results[9], results[10], results[11], results[12], results[13], results[14], results[15], results[16], results[17], results[18], results[19])
```

```python
import functools

import jax
import jax.numpy as jnp
from jax import lax
from jax.experimental import pallas as pl
from jax.experimental.pallas import tpu as pltpu
from jax.sharding import PartitionSpec as P

D = 896
HEADS = 14
KV_HEADS = 2
HEAD = 64
ATT = 896
GROUP = 7
KVW = KV_HEADS * HEAD

norm_eps = 1e-06
rope_base = 1000000.0
plus_token = 10
minus_token = 12
clip_limit = 0.05
beta_one = 0.9
beta_two = 0.95
adam_eps = 1e-08
decay_rate = 0.1
rates = (0.03, 0.015, 0.015, 0.015, 0.0015, 0.3)

MESH = pl.DeviceIdType.MESH
f32 = jnp.float32
bf16 = jnp.bfloat16


def exchange_kernel(hid_count, wide_count, modes, *refs):
    count = len(modes)
    ins, outs = refs[:count], refs[count : 2 * count]
    send_sems, recv_sems, local_sems = refs[2 * count :]
    h = lax.axis_index("hid")
    w = lax.axis_index("wide")
    me = h * wide_count + w
    total = hid_count * wide_count
    barrier = pltpu.get_barrier_semaphore()

    def greet(k, carry):
        other = lax.rem(me + k, total)
        pl.semaphore_signal(
            barrier, inc=1, device_id=(other // wide_count, other % wide_count), device_id_type=MESH
        )
        return carry

    lax.fori_loop(1, total, greet, 0)
    pl.semaphore_wait(barrier, total - 1)
    for i, (mode, group) in enumerate(modes):
        size = {"all": total, "wide": wide_count, "hid": hid_count}[group]
        mine = {"all": me, "wide": w, "hid": h}[group]

        def start(k, carry, i=i, mode=mode, group=group, size=size, mine=mine):
            other = lax.rem(mine + k, size)
            target = {
                "all": (other // wide_count, other % wide_count),
                "wide": (h, other),
                "hid": (other, w),
            }[group]
            pltpu.make_async_remote_copy(
                src_ref=ins[i].at[other] if mode == "a2a" else ins[i],
                dst_ref=outs[i].at[mine],
                send_sem=send_sems.at[i],
                recv_sem=recv_sems.at[i],
                device_id=target,
                device_id_type=MESH,
            ).start()
            return carry

        lax.fori_loop(1, size, start, 0)
        pltpu.make_async_copy(
            ins[i].at[mine] if mode == "a2a" else ins[i], outs[i].at[mine], local_sems.at[i]
        ).start()
    for i, (mode, group) in enumerate(modes):
        size = {"all": total, "wide": wide_count, "hid": hid_count}[group]
        mine = {"all": me, "wide": w, "hid": h}[group]
        rest = outs[i].at[pl.ds(0, size - 1)]
        pltpu.make_async_copy(
            ins[i].at[mine] if mode == "a2a" else ins[i], outs[i].at[mine], local_sems.at[i]
        ).wait()
        pltpu.make_async_copy(rest, rest, send_sems.at[i]).wait()
        pltpu.make_async_copy(rest, rest, recv_sems.at[i]).wait()


def exchange(ident, *items):
    hid_count = lax.axis_size("hid")
    wide_count = lax.axis_size("wide")
    sizes = {"all": hid_count * wide_count, "wide": wide_count, "hid": hid_count}
    modes = tuple((mode, group) for _, mode, group in items)
    shapes = [
        jax.ShapeDtypeStruct(
            item.shape if mode == "a2a" else (sizes[group],) + item.shape, item.dtype
        )
        for item, mode, group in items
    ]
    count = len(items)
    return pl.pallas_call(
        functools.partial(exchange_kernel, hid_count, wide_count, modes),
        out_shape=shapes,
        in_specs=[pl.BlockSpec(memory_space=pl.ANY)] * count,
        out_specs=[pl.BlockSpec(memory_space=pl.ANY)] * count,
        scratch_shapes=[pltpu.SemaphoreType.DMA((count,))] * 3,
        compiler_params=pltpu.CompilerParams(collective_id=ident, has_side_effects=True),
        name="exchange_%d" % ident,
    )(*[item for item, _, _ in items])


def dot(a, b, spec):
    return jnp.einsum(spec, a, b, preferred_element_type=f32)


def rms_r(rows):
    return lax.rsqrt(jnp.mean(rows * rows, axis=-1, keepdims=True) + norm_eps)


def rms_back(x, gain, dy):
    r = rms_r(x)
    dx = r * gain * dy - x * (r * r * r) * jnp.mean(x * gain * dy, axis=-1, keepdims=True)
    return dx, jnp.sum(dy * x * r, axis=0)


def rotate(values, cosine, sine):
    half = HEAD // 2
    a, b = values[..., :half], values[..., half:]
    return jnp.concatenate([a * cosine - b * sine, b * cosine + a * sine], axis=-1)


def per_device(
    token_ids,
    segment_ids,
    step_ends,
    step_labels,
    step_count,
    table,
    attn_in,
    attn_out,
    mlp_in,
    mlp_out,
    small_params,
    table_first,
    attn_in_first,
    attn_out_first,
    mlp_in_first,
    mlp_out_first,
    small_first,
    table_second,
    attn_in_second,
    attn_out_second,
    mlp_in_second,
    mlp_out_second,
    small_second,
):
    h = lax.axis_index("hid")
    w = lax.axis_index("wide")
    hid_count = lax.axis_size("hid")
    wide_count = lax.axis_size("wide")
    total = hid_count * wide_count
    me = h * wide_count + w
    micro, group_seqs, seq_len = token_ids.shape
    slots = step_ends.shape[2]
    picks = micro * slots
    tokens = micro * seq_len
    block_rows = table.shape[0]
    cap = 2 * seq_len // wide_count
    d_local = attn_in.shape[0]
    in_cols = attn_in.shape[1]
    out_cols = attn_out.shape[1]
    ff_part = mlp_in.shape[2] // wide_count
    small_local = small_params.shape[0]
    ranks = micro * cap

    ids_labels = jnp.concatenate([token_ids, step_labels], axis=2)
    ids_labels = ids_labels.reshape(micro * group_seqs, seq_len + slots)
    small_send = jnp.pad(small_params.astype(bf16).astype(f32), (0, 128 - small_local))[None]
    mlp_low = jnp.concatenate(
        [
            mlp_in.astype(bf16).reshape(d_local, 2, wide_count, ff_part).transpose(2, 0, 1, 3).reshape(
                wide_count, d_local, 2 * ff_part
            ),
            mlp_out.astype(bf16).reshape(wide_count, ff_part, d_local).transpose(0, 2, 1),
        ],
        axis=2,
    )
    il_all, small_all = exchange(0, (ids_labels, "ag", "hid"), (small_send, "ag", "all"))
    il_all = il_all.reshape(hid_count, micro, group_seqs, seq_len + slots).transpose(1, 0, 2, 3)
    il_all = il_all.reshape(micro, total, seq_len + slots)
    ids_all = il_all[:, :, :seq_len]
    labels_all = il_all[:, :, seq_len:]
    smalls = small_all[:, 0, :small_local].reshape(-1)
    gains = smalls[: 3 * D].reshape(3, D)
    bias = smalls[3 * D :]
    in_low = lax.all_gather(attn_in.astype(bf16), ("hid", "wide"))
    out_low = lax.all_gather(attn_out.astype(bf16), ("hid", "wide"))
    w_in = in_low.reshape(hid_count, D, in_cols).transpose(1, 0, 2).reshape(D, hid_count * in_cols)
    w_out = out_low.reshape(hid_count, ATT, out_cols).transpose(1, 0, 2).reshape(ATT, D)

    mine = ids_all // block_rows == me
    rank_mine = jnp.cumsum(mine.astype(jnp.int32), axis=2) - 1
    slot_iota = jnp.arange(cap, dtype=jnp.int32)
    hit = mine[:, :, None, :] & (rank_mine[:, :, None, :] == slot_iota[None, None, :, None])
    slot_row = jnp.sum(
        jnp.where(hit, (ids_all - me * block_rows)[:, :, None, :] + 1, 0), axis=3
    ) - 1
    slot_row = slot_row.transpose(1, 0, 2).reshape(total * ranks)
    send_rows = table[jnp.maximum(slot_row, 0)].astype(bf16).reshape(total, ranks, D)
    recv_rows, w_all = exchange(1, (send_rows, "a2a", "all"), (mlp_low, "a2a", "wide"))
    w_all = w_all.reshape(D, 3 * ff_part)

    own_ids = lax.dynamic_slice_in_dim(token_ids, w, 1, 1)[:, 0]
    own_block = own_ids // block_rows
    earlier = jnp.tril(jnp.ones((seq_len, seq_len), bool), -1)
    own_rank = jnp.sum(
        (own_block[:, :, None] == own_block[:, None, :]) & earlier[None], axis=2, dtype=jnp.int32
    )
    place = own_block * ranks + jnp.arange(micro, dtype=jnp.int32)[:, None] * cap + own_rank
    place = place.reshape(tokens)
    select = (place[:, None] == jnp.arange(total * ranks, dtype=jnp.int32)[None, :]).astype(bf16)
    embedded = dot(select, recv_rows.reshape(total * ranks, D), "tr,rd->td")
    segment = segment_ids[:, 0]
    ends = step_ends[:, 0]
    same = segment[:, :, None] == segment[:, None, :]
    position = jnp.sum(same & earlier[None], axis=2).astype(f32)
    frequency = rope_base ** (-jnp.arange(HEAD // 2, dtype=f32) / (HEAD // 2))
    angle = position[:, :, None] * frequency
    cosine, sine = jnp.cos(angle), jnp.sin(angle)
    cos_p = jnp.take_along_axis(cosine, ends[:, :, None], axis=1)
    sin_p = jnp.take_along_axis(sine, ends[:, :, None], axis=1)
    places = jnp.arange(seq_len, dtype=jnp.int32)
    seg_p = jnp.take_along_axis(segment, ends, axis=1)
    allowed = (seg_p[:, :, None] == segment[:, None, :]) & (places[None, None] <= ends[:, :, None])
    pick_at = (jnp.arange(micro, dtype=jnp.int32)[:, None] * seq_len + ends).reshape(picks)

    normed_one = (embedded * rms_r(embedded) * gains[0]).astype(bf16)
    emb_p = embedded[pick_at]
    n1_p = normed_one[pick_at]
    kv = dot(normed_one, w_in[:, ATT:], "td,dc->tc") + bias[ATT:]
    keys = rotate(kv[:, :KVW].reshape(micro, seq_len, KV_HEADS, HEAD), cosine[:, :, None], sine[:, :, None])
    keys = keys.astype(bf16)
    values = kv[:, KVW:].reshape(micro, seq_len, KV_HEADS, HEAD).astype(bf16)
    q = dot(n1_p, w_in[:, :ATT], "td,dc->tc") + bias[:ATT]
    queries = rotate(q.reshape(micro, slots, HEADS, HEAD), cos_p[:, :, None], sin_p[:, :, None])
    queries = queries.astype(bf16).reshape(micro, slots, KV_HEADS, GROUP, HEAD)
    scores = dot(queries, keys, "mskgd,mtkd->mkgst") * HEAD ** (-0.5)
    scores = jnp.where(allowed[:, None, None], scores, -1e30)
    probs = jax.nn.softmax(scores, axis=-1)
    probs_low = probs.astype(bf16)
    mixed = dot(probs_low, values, "mkgst,mtkd->mskgd").reshape(picks, ATT).astype(bf16)
    hidden_one = emb_p + dot(mixed, w_out, "ta,ad->td")
    n2 = (hidden_one * rms_r(hidden_one) * gains[1]).astype(bf16)

    (n2_all,) = exchange(2, (n2, "ag", "all"))
    n2_all = n2_all.reshape(total * picks, D)
    gate_up = dot(n2_all, w_all[:, : 2 * ff_part], "rd,df->rf")
    gate, upward = gate_up[:, :ff_part], gate_up[:, ff_part:]
    sig = jax.nn.sigmoid(gate)
    inner = (gate * sig * upward).astype(bf16)
    down_part = dot(inner, w_all[:, 2 * ff_part :], "rf,df->rd").astype(bf16)
    (down_recv,) = exchange(3, (down_part.reshape(total, picks, D), "a2a", "all"))
    hidden_two = hidden_one + jnp.sum(down_recv.astype(f32), axis=0)
    final = (hidden_two * rms_r(hidden_two) * gains[2]).astype(bf16)

    (final_all,) = exchange(4, (final, "ag", "all"))
    final_all = final_all.reshape(total * picks, D)
    table_low = table.astype(bf16)
    logits = dot(final_all, table_low, "rd,vd->rv")
    global_of = me * block_rows + jnp.arange(block_rows, dtype=jnp.int32)
    local_max = jnp.max(logits, axis=1)
    local_sum = jnp.sum(jnp.exp(logits - local_max[:, None]), axis=1)
    plus_value = jnp.sum(jnp.where((global_of == plus_token)[None], logits, 0.0), axis=1)
    minus_value = jnp.sum(jnp.where((global_of == minus_token)[None], logits, 0.0), axis=1)
    labels = labels_all.transpose(1, 0, 2).reshape(total * picks)
    live = labels >= 0
    target_value = jnp.where(labels >= 1, plus_value, minus_value)
    stats = jnp.stack([local_max, local_sum, target_value])
    (stats_all,) = exchange(5, (stats, "ag", "all"))
    top = jnp.max(stats_all[:, 0], axis=0)
    summed = jnp.sum(stats_all[:, 1] * jnp.exp(stats_all[:, 0] - top[None]), axis=0)
    log_sum = top + jnp.log(summed)
    loss_total = jnp.sum(jnp.where(live, log_sum - jnp.sum(stats_all[:, 2], axis=0), 0.0))
    count_total = jnp.sum(live.astype(f32))
    target_global = jnp.where(labels >= 1, plus_token, minus_token)
    onehot = ((global_of[None, :] == target_global[:, None]) & live[:, None]).astype(f32)
    dlogits = (
        jnp.where(live[:, None], jnp.exp(logits - log_sum[:, None]), 0.0) - onehot
    ).astype(bf16)
    dfinal_part = dot(dlogits, table_low, "rv,vd->rd").astype(bf16)
    (dfinal_recv,) = exchange(6, (dfinal_part.reshape(total, picks, D), "a2a", "all"))
    dfinal = jnp.sum(dfinal_recv.astype(f32), axis=0)
    dh2, dgain_three = rms_back(hidden_two, gains[2], dfinal)
    dmix = dh2.astype(bf16)

    (dmix_all,) = exchange(7, (dmix, "ag", "all"))
    dmix_all = dmix_all.reshape(total * picks, D)
    dinner = dot(dmix_all, w_all[:, 2 * ff_part :], "rd,df->rf")
    dgate = dinner * upward * sig * (1.0 + gate * (1.0 - sig))
    dupward = dinner * gate * sig
    dgu = jnp.concatenate([dgate, dupward], axis=1).astype(bf16)
    dn2_part = dot(dgu, w_all[:, : 2 * ff_part], "rf,df->rd").astype(bf16)
    mlp_grad = jnp.concatenate(
        [dot(n2_all, dgu, "rd,rf->df"), dot(dmix_all, inner, "rd,rf->df")], axis=1
    ).astype(bf16)
    dn2_recv, mlp_recv = exchange(
        8,
        (dn2_part.reshape(total, picks, D), "a2a", "all"),
        (mlp_grad.reshape(wide_count, d_local, 3 * ff_part), "a2a", "wide"),
    )
    dn2 = jnp.sum(dn2_recv.astype(f32), axis=0)
    dx, dgain_two = rms_back(hidden_one, gains[1], dn2)
    dh1 = dh2 + dx

    dbranch = dh1.astype(bf16)
    dmixed = dot(dbranch, w_out, "td,ad->ta").astype(bf16).reshape(micro, slots, KV_HEADS, GROUP, HEAD)
    dprobs = dot(dmixed, values, "mskgd,mtkd->mkgst")
    dvalues = dot(probs_low, dmixed, "mkgst,mskgd->mtkd")
    dscores = (
        probs * (dprobs - jnp.sum(dprobs * probs, axis=-1, keepdims=True)) * HEAD ** (-0.5)
    ).astype(bf16)
    dq = dot(dscores, keys, "mkgst,mtkd->mskgd").reshape(micro, slots, HEADS, HEAD)
    dk = dot(dscores, queries, "mkgst,mskgd->mtkd")
    dq = rotate(dq, cos_p[:, :, None], -sin_p[:, :, None]).reshape(picks, ATT).astype(bf16)
    dk = rotate(dk, cosine[:, :, None], -sine[:, :, None]).reshape(tokens, KVW)
    dkv = jnp.concatenate([dk, dvalues.reshape(tokens, KVW)], axis=1).astype(bf16)
    bias_grad = jnp.concatenate(
        [jnp.sum(dq.astype(f32), axis=0), jnp.sum(dkv.astype(f32), axis=0)]
    )
    kv_grad = dot(normed_one, dkv, "td,tc->dc").astype(bf16)
    pick_hot = (jnp.arange(tokens, dtype=jnp.int32)[:, None] == pick_at[None, :]).astype(f32)
    dn1_p = dot(dq, w_in[:, :ATT], "tc,dc->td")
    spread = jnp.einsum(
        "tp,pd->td",
        pick_hot,
        jnp.concatenate([dn1_p, dh1], axis=1),
        precision=lax.Precision.HIGHEST,
    )
    dn1 = dot(dkv, w_in[:, ATT:], "tc,dc->td") + spread[:, :D]
    dx, dgain_one = rms_back(embedded, gains[0], dn1)
    dembedded = (spread[:, D:] + dx).astype(bf16)

    demb_send = dot(select, dembedded, "tr,td->rd").astype(bf16).reshape(total, ranks, D)
    dq_wide = jnp.pad(dq, ((0, 0), (0, 2 * KVW))).reshape(picks, hid_count, 1, in_cols)
    db_wide = dbranch.reshape(picks, hid_count, 1, out_cols)

    def spread_to(rows, dims):
        return jnp.broadcast_to(rows, (picks, hid_count, wide_count, dims))

    grads_send = jnp.concatenate(
        [
            spread_to(dq_wide, in_cols),
            spread_to(db_wide, out_cols),
            spread_to(n1_p.reshape(picks, 1, wide_count, d_local), d_local),
            spread_to(mixed.reshape(picks, 1, wide_count, d_local), d_local),
        ],
        axis=3,
    )
    grads_send = grads_send.transpose(1, 2, 0, 3).reshape(total, picks, -1)
    small_grad = jnp.concatenate([dgain_one, dgain_two, dgain_three, bias_grad])
    small_grad = jnp.pad(small_grad.reshape(total, 1, small_local), ((0, 0), (0, 0), (0, 128 - small_local)))
    demb_recv, rows_recv, kv_recv, small_recv = exchange(
        9,
        (demb_send, "a2a", "all"),
        (grads_send, "a2a", "all"),
        (kv_grad.reshape(wide_count, d_local, 2 * KVW), "a2a", "wide"),
        (small_grad, "a2a", "all"),
    )
    rows_recv = rows_recv.reshape(total * picks, -1)
    c0, c1, c2 = in_cols, in_cols + out_cols, in_cols + out_cols + d_local
    in_g = dot(rows_recv[:, c1:c2], rows_recv[:, :c0], "rd,rc->dc")
    out_g = dot(rows_recv[:, c2:], rows_recv[:, c0:c1], "ra,rd->ad")
    kv_sum = jnp.sum(kv_recv.astype(f32), axis=0)
    table_g = dot(dlogits, final_all, "rv,rd->vd") + dot(
        (slot_row[:, None] == jnp.arange(block_rows, dtype=jnp.int32)[None, :]).astype(bf16),
        demb_recv.reshape(total * ranks, D),
        "rv,rd->vd",
    )
    (kv_all,) = exchange(10, (kv_sum, "ag", "hid"))
    kv_full = jnp.pad(jnp.sum(kv_all, axis=0), ((0, 0), (ATT, 0)))
    in_g = in_g + lax.dynamic_slice_in_dim(kv_full, h * in_cols, in_cols, 1)
    mlp_g = mlp_recv.astype(f32)
    gate_g = (
        mlp_g[:, :, : 2 * ff_part]
        .reshape(wide_count, d_local, 2, ff_part)
        .transpose(1, 2, 0, 3)
        .reshape(d_local, 2, wide_count * ff_part)
    )
    down_g = mlp_g[:, :, 2 * ff_part :].transpose(0, 2, 1).reshape(wide_count * ff_part, d_local)
    small_g = jnp.sum(small_recv[:, 0, :small_local], axis=0)
    totals = (table_g, in_g, out_g, gate_g, down_g, small_g)
    sum_squares = sum((jnp.sum(item * item) for item in totals))
    (squares_all,) = exchange(11, (jnp.full((1, 128), sum_squares), "ag", "all"))
    squares = jnp.sum(squares_all[:, 0, 0])

    denom = jnp.maximum(count_total, 1.0)
    grad_norm = jnp.sqrt(squares) / denom
    factor = clip_limit / jnp.maximum(grad_norm, clip_limit)
    step_value = step_count.astype(f32)
    bias_one = 1.0 - beta_one**step_value
    bias_two = 1.0 - beta_two**step_value
    masters = (table, attn_in, attn_out, mlp_in, mlp_out, small_params)
    firsts = (table_first, attn_in_first, attn_out_first, mlp_in_first, mlp_out_first, small_first)
    seconds = (
        table_second,
        attn_in_second,
        attn_out_second,
        mlp_in_second,
        mlp_out_second,
        small_second,
    )
    results = [loss_total / denom, grad_norm]
    for grad_total, weight_old, first_old, second_old, step_rate in zip(
        totals, masters, firsts, seconds, rates
    ):
        clipped = grad_total / denom * factor
        first_new = beta_one * first_old + (1.0 - beta_one) * clipped
        second_new = beta_two * second_old + (1.0 - beta_two) * clipped * clipped
        update = (
            first_new / bias_one / (jnp.sqrt(second_new / bias_two) + adam_eps)
            + decay_rate * weight_old
        )
        results += [weight_old - step_rate * update, first_new, second_new]
    return tuple(results)


def solution(mesh):
    in_specs = (
        P(None, "hid", None),
        P(None, ("hid", "wide"), None),
        P(None, ("hid", "wide"), None),
        P(None, "hid", None),
        P(),
        P(("hid", "wide"), None),
        P("wide", "hid"),
        P("wide", "hid"),
        P("wide", None, "hid"),
        P("hid", "wide"),
        P(("hid", "wide")),
        P(("hid", "wide"), None),
        P("wide", "hid"),
        P("wide", "hid"),
        P("wide", None, "hid"),
        P("hid", "wide"),
        P(("hid", "wide")),
        P(("hid", "wide"), None),
        P("wide", "hid"),
        P("wide", "hid"),
        P("wide", None, "hid"),
        P("hid", "wide"),
        P(("hid", "wide")),
    )
    out_specs = (
        P(),
        P(),
        P(("hid", "wide"), None),
        P(("hid", "wide"), None),
        P(("hid", "wide"), None),
        P("wide", "hid"),
        P("wide", "hid"),
        P("wide", "hid"),
        P("wide", "hid"),
        P("wide", "hid"),
        P("wide", "hid"),
        P("wide", None, "hid"),
        P("wide", None, "hid"),
        P("wide", None, "hid"),
        P("hid", "wide"),
        P("hid", "wide"),
        P("hid", "wide"),
        P(("hid", "wide")),
        P(("hid", "wide")),
        P(("hid", "wide")),
    )
    return jax.shard_map(
        per_device, mesh=mesh, in_specs=in_specs, out_specs=out_specs, check_vma=False
    )
```
